128 devices in a mesh: dom: 16 (over x, y), sub: 8 (over z, core).
Axes of the slice: x: 4, y: 4, z: 4, core: 2. Of those that a mesh axis runs over, the one named last changes fastest.
Arguments:
- features: bfloat16 [131072, 602], P(('dom', 'sub')), may hold values from -6 to 6
- w_inner: bfloat16 [602, 256], replicated, may hold values from -0.25 to 0.25
- bias_inner: float32 [256], replicated, may hold values from -6 to 6
- w_outer: bfloat16 [256, 41], replicated, may hold values from -0.375 to 0.375
- bias_outer: float32 [41], replicated, may hold values from -6 to 6
- tiles: bfloat16 [1024, 32, 128, 128], P(('dom', 'sub')), may hold values from -3 to 3
- tile_col: int32 [1024, 32], P(('dom', 'sub')), may hold values from 0 to 135, as said below
- degrees: int32 [131072], P(('dom', 'sub')), may hold values from 1 to 32
- send_rows: int32 [128, 128, 128], P(('dom', 'sub')), may hold values from -1 to 1023, as said below
Outputs:
- logits: float32 [131072, 41], P(('dom', 'sub'))
The draws below stay inside these ranges and needn't reach their ends.
Inputs may be any that keep to these rules, and one draw needn't show every extreme that they name: send_rows[e, p, s] is the row, among device e's 1024 vertices, that fills slot s of e's list for device p, or -1 for an unused slot; live slots come first and every list has 1 to 128 live slots; every sender has a full list, and in every draw some device receives full lists from all senders. tile_col[d * 8 + r, t] is the column block, in device d's column space, of tile t of row block r; the 32 column blocks of a row block are distinct.
All inputs are finite; a program needn't handle non-finite values.
Results may differ from the reference program's by a relative error of at most 0.0042.
Values may be sent and summed in bfloat16 or wider, within the bound.
No kernel may reach another device: no remote copies, remote signals or barrier semaphores. Data moves between devices by JAX's collectives and lax.ppermute only.
A program may use at most 128 MiB of HBM per device.

```python
import jax
import jax.numpy as jnp
from jax import lax

F_IN = 602
HID = 256
CLASSES = 41
BLK = 128
TILES = 32
V_DEV = 1024
PEERS = 128
ROW_BLOCKS = 8
COL_BLOCKS = 136
VERTS = 131072


def draw_send_rows(key, part):
    key_rows = jax.random.fold_in(key, 11)
    key_counts = jax.random.fold_in(key, 12)
    key_full = jax.random.fold_in(key, 13)
    key_target = jax.random.fold_in(key, 14)
    picked = jax.random.randint(key_rows, (PEERS, PEERS, BLK), 0, V_DEV)
    counts = jax.random.randint(key_counts, (PEERS, PEERS), 1, BLK + 1)
    full_peer = jax.random.randint(key_full, (PEERS,), 0, PEERS)
    target = jax.random.randint(key_target, (), 0, PEERS)
    peer_ids = jnp.arange(PEERS)
    counts = jnp.where(peer_ids[None, :] == full_peer[:, None], BLK, counts)
    counts = jnp.where(peer_ids[None, :] == target, BLK, counts)
    slots = jnp.arange(BLK)
    return jnp.where(slots[None, None, :] < counts[:, :, None], picked, -1).astype(jnp.int32)


def draw_tile_col(key, part):
    keys = jax.random.split(jax.random.fold_in(key, 21), PEERS)
    orders = jax.vmap(lambda single: jax.random.permutation(single, COL_BLOCKS))(keys)
    flat = jnp.arange(ROW_BLOCKS * TILES) % COL_BLOCKS
    picked = orders[:, flat]
    return picked.reshape(PEERS * ROW_BLOCKS, TILES).astype(jnp.int32)


def place_ends(drawn, stream_key, least, top_value):
    index_at = [jax.random.randint(jax.random.fold_in(stream_key, axis), (), 0, length) for axis, length in enumerate(drawn.shape)]
    main_axis = drawn.shape.index(max(drawn.shape))
    beside = index_at[:main_axis] + [(index_at[main_axis] + 1) % drawn.shape[main_axis]] + index_at[main_axis + 1:]
    return drawn.at[tuple(index_at)].set(least).at[tuple(beside)].set(top_value)


def levels(rng, dims, shards, low, largest):
    def one(position, blocks):
        draws = jax.random.uniform(jax.random.fold_in(jax.random.fold_in(rng, 6), position), (blocks,), jnp.float32, low / len(shards), largest / len(shards))
        return jnp.repeat(jnp.exp(draws), dims[position] // blocks).reshape((-1,) + (1,) * (len(dims) - position - 1))

    gain = one(*shards[0])
    for cut in shards[1:]:
        gain = gain * one(*cut)
    return gain


def centred(stream_key, extent, scale, reach, cuts=(), kind=jnp.bfloat16):
    drawn = scale * jax.random.normal(stream_key, extent, jnp.float32)
    if cuts:
        drawn = drawn * levels(stream_key, extent, cuts, -0.22, 0.18)
    return jnp.clip(drawn, -reach, reach).astype(kind)


def setup_inputs(seed: int = 0) -> dict:
    key_of = jax.random.split(jax.random.key(seed), 10)
    return {
        "features": centred(key_of[0], (VERTS, F_IN), 1.0, 6.0, ((0, 128),)),
        "w_inner": centred(key_of[1], (F_IN, HID), F_IN ** -0.5, 0.25),
        "bias_inner": centred(key_of[2], (HID,), 1.0, 6.0, (), jnp.float32),
        "w_outer": centred(key_of[3], (HID, CLASSES), HID ** -0.5, 0.375),
        "bias_outer": centred(key_of[4], (CLASSES,), 1.0, 6.0, (), jnp.float32),
        "tiles": centred(key_of[5], (PEERS * ROW_BLOCKS, TILES, BLK, BLK), (12.0 / (TILES * BLK) ** 0.5), 3.0, ((0, 128),)),
        "tile_col": draw_tile_col(jax.random.fold_in(key_of[9], 71), 0),
        "degrees": place_ends(jax.random.randint(key_of[7], (VERTS,), 1, 33), jax.random.fold_in(key_of[7], 1), 1, 32).astype(jnp.int32),
        "send_rows": draw_send_rows(jax.random.fold_in(key_of[9], 71), 0),
    }


def aggregate(feature_rows, tiles, tile_col, send_rows):
    width = feature_rows.shape[1]
    by_device = feature_rows.reshape(PEERS, V_DEV, width)
    tile_sets = tiles.reshape(PEERS, ROW_BLOCKS, TILES, BLK, BLK)
    col_sets = tile_col.reshape(PEERS, ROW_BLOCKS, TILES)

    def per_target(target):
        slot_rows = lax.dynamic_index_in_dim(send_rows, target, 1, keepdims=False)
        clipped = jnp.clip(slot_rows, 0, V_DEV - 1).astype(jnp.int32)
        fetched = jnp.take_along_axis(by_device, clipped[:, :, None], axis=1)
        fetched = jnp.where((slot_rows >= 0)[:, :, None], fetched, jnp.zeros((), feature_rows.dtype))
        own_rows = lax.dynamic_index_in_dim(by_device, target, 0, keepdims=False)
        columns = jnp.concatenate([own_rows.reshape(ROW_BLOCKS, BLK, width), fetched], axis=0)
        target_tiles = lax.dynamic_index_in_dim(tile_sets, target, 0, keepdims=False)
        target_cols = lax.dynamic_index_in_dim(col_sets, target, 0, keepdims=False)
        blocks = columns[target_cols]
        summed = jnp.einsum('rtij,rtjw->riw', target_tiles.astype(jnp.float32), blocks.astype(jnp.float32))
        return summed.reshape(V_DEV, width)
    results = lax.map(per_target, jnp.arange(PEERS, dtype=jnp.int32))
    return results.reshape(PEERS * V_DEV, width)

def reference(features, w_inner, bias_inner, w_outer, bias_outer, tiles, tile_col, degrees, send_rows):
    inv_sqrt = lax.rsqrt(degrees.astype(jnp.float32))[:, None]
    projected = (jnp.dot(features, w_inner, preferred_element_type=jnp.float32) * inv_sqrt).astype(jnp.bfloat16)
    agg_inner = aggregate(projected, tiles, tile_col, send_rows)
    hidden = (inv_sqrt * jax.nn.relu(inv_sqrt * agg_inner + bias_inner)).astype(jnp.bfloat16)
    scores = jnp.dot(hidden, w_outer, preferred_element_type=jnp.float32).astype(jnp.bfloat16)
    agg_outer = aggregate(scores, tiles, tile_col, send_rows)
    return inv_sqrt * agg_outer + bias_outer
```

```python
import functools

import jax
import jax.numpy as jnp
from jax import lax
from jax.experimental import pallas as pl
from jax.experimental.pallas import tpu as pltpu
from jax.sharding import PartitionSpec as P

BLOCK = 128
PEER_STEP = 8


def gather_rows_kernel(lists_ref, rows_ref, out_ref):
    height = rows_ref.shape[0]
    by_slot = lists_ref[...].T
    row_of_lane = lax.broadcasted_iota(jnp.int32, (BLOCK, height), 1)
    rows = rows_ref[...]
    for p in range(PEER_STEP):
        pick = (by_slot[:, p : p + 1] == row_of_lane).astype(jnp.float32).astype(jnp.bfloat16)
        out_ref[p] = jnp.dot(pick, rows, preferred_element_type=jnp.float32).astype(jnp.bfloat16)


def gather_rows(lists, rows):
    peers = lists.shape[0]
    height, width = rows.shape
    return pl.pallas_call(
        gather_rows_kernel,
        grid=(peers // PEER_STEP,),
        in_specs=[
            pl.BlockSpec((PEER_STEP, BLOCK), lambda g: (g, 0)),
            pl.BlockSpec((height, width), lambda g: (0, 0)),
        ],
        out_specs=pl.BlockSpec((PEER_STEP, BLOCK, width), lambda g: (g, 0, 0)),
        out_shape=jax.ShapeDtypeStruct((peers, BLOCK, width), jnp.bfloat16),
        name="gather_rows",
    )(lists, rows)


def inner_kernel(
    cols_ref, tiles_ref, own_ref, arrived_ref, inv_ref, bias_ref, w_ref, out_ref, space, sems
):
    step = pl.program_id(0)
    own_blocks = own_ref.shape[0]

    @pl.when(step == 0)
    def _():
        far = pltpu.make_async_copy(arrived_ref, space.at[pl.ds(own_blocks, arrived_ref.shape[0])], sems.at[0])
        near = pltpu.make_async_copy(own_ref, space.at[pl.ds(0, own_blocks)], sems.at[1])
        far.start()
        near.start()
        near.wait()
        far.wait()

    total = jnp.zeros(space.shape[1:], jnp.float32)
    for t in range(0, tiles_ref.shape[1], 2):
        left = jnp.concatenate([tiles_ref[0, t], tiles_ref[0, t + 1]], axis=1)
        right = jnp.concatenate([space[cols_ref[step, t]], space[cols_ref[step, t + 1]]], axis=0)
        total = total + jnp.dot(left, right, preferred_element_type=jnp.float32)
    inv = inv_ref[...]
    hidden = (inv * jnp.maximum(inv * total + bias_ref[...], 0.0)).astype(jnp.bfloat16)
    out_ref[...] = lax.dot_general(
        w_ref[...], hidden, (((1,), (1,)), ((), ())), preferred_element_type=jnp.float32
    ).astype(jnp.bfloat16)


def inner_aggregate(tile_col, tiles, own, arrived, inv_col, bias, w_t):
    row_blocks, count, _, _ = tiles.shape
    width = own.shape[-1]
    peers = arrived.shape[0]
    return pl.pallas_call(
        inner_kernel,
        grid_spec=pltpu.PrefetchScalarGridSpec(
            num_scalar_prefetch=1,
            grid=(row_blocks,),
            in_specs=[
                pl.BlockSpec((1, count, BLOCK, BLOCK), lambda g, c: (g, 0, 0, 0)),
                pl.BlockSpec(memory_space=pl.ANY),
                pl.BlockSpec(memory_space=pl.ANY),
                pl.BlockSpec((BLOCK, 1), lambda g, c: (g, 0)),
                pl.BlockSpec((1, width), lambda g, c: (0, 0)),
                pl.BlockSpec(w_t.shape, lambda g, c: (0, 0)),
            ],
            out_specs=pl.BlockSpec((w_t.shape[0], BLOCK), lambda g, c: (0, g)),
            scratch_shapes=[
                pltpu.VMEM((row_blocks + peers, BLOCK, width), jnp.bfloat16),
                pltpu.SemaphoreType.DMA((2,)),
            ],
        ),
        out_shape=jax.ShapeDtypeStruct((w_t.shape[0], row_blocks * BLOCK), jnp.bfloat16),
        name="inner_aggregate",
    )(tile_col, tiles, own, arrived, inv_col, bias, w_t)


def gather_scores_kernel(lists_ref, stacked_ref, out_ref):
    quarter_rows = stacked_ref.shape[1]
    classes = out_ref.shape[1]
    stacked = stacked_ref[...]
    row_of_sublane = lax.broadcasted_iota(jnp.int32, (quarter_rows, 2 * BLOCK), 0)
    for p in range(0, PEER_STEP, 2):
        index = jnp.concatenate([lists_ref[p : p + 1], lists_ref[p + 1 : p + 2]], axis=1)
        low = jnp.bitwise_and(index, quarter_rows - 1)
        quarter = jnp.right_shift(index, quarter_rows.bit_length() - 1)
        pick = (low == row_of_sublane).astype(jnp.float32).astype(jnp.bfloat16)
        every = jnp.dot(stacked, pick, preferred_element_type=jnp.float32)
        chosen = jnp.zeros((classes, 2 * BLOCK), jnp.float32)
        for q in range(stacked_ref.shape[0] // classes):
            chosen = jnp.where(quarter == q, every[q * classes : (q + 1) * classes], chosen)
        chosen = chosen.astype(jnp.bfloat16)
        out_ref[p] = chosen[:, :BLOCK]
        out_ref[p + 1] = chosen[:, BLOCK:]


def gather_scores(lists, scores_t):
    peers = lists.shape[0]
    classes, height = scores_t.shape
    quarters = height // 256
    stacked = scores_t.reshape(classes, quarters, 256).transpose(1, 0, 2).reshape(quarters * classes, 256)
    return pl.pallas_call(
        gather_scores_kernel,
        grid=(peers // PEER_STEP,),
        in_specs=[
            pl.BlockSpec((PEER_STEP, BLOCK), lambda g: (g, 0)),
            pl.BlockSpec(stacked.shape, lambda g: (0, 0)),
        ],
        out_specs=pl.BlockSpec((PEER_STEP, classes, BLOCK), lambda g: (g, 0, 0)),
        out_shape=jax.ShapeDtypeStruct((peers, classes, BLOCK), jnp.bfloat16),
        name="gather_scores",
    )(lists, stacked)


def outer_kernel(cols_ref, tiles_ref, own_ref, arrived_ref, inv_ref, bias_ref, out_ref, space):
    step = pl.program_id(0)
    own_blocks = tiles_ref.shape[1] and own_ref.shape[1] // BLOCK

    @pl.when(step == 0)
    def _():
        for b in range(own_blocks):
            space[b] = own_ref[:, b * BLOCK : (b + 1) * BLOCK]
        space[own_blocks:] = arrived_ref[...]

    total = jnp.zeros(out_ref.shape, jnp.float32)
    for t in range(0, tiles_ref.shape[1], 2):
        right = jnp.concatenate([tiles_ref[0, t], tiles_ref[0, t + 1]], axis=1)
        left = jnp.concatenate([space[cols_ref[step, t]], space[cols_ref[step, t + 1]]], axis=1)
        total = total + lax.dot_general(
            left, right, (((1,), (1,)), ((), ())), preferred_element_type=jnp.float32
        )
    out_ref[...] = inv_ref[...] * total + bias_ref[...]


def outer_aggregate(tile_col, tiles, own_t, arrived, inv_row, bias_col):
    row_blocks, count, _, _ = tiles.shape
    classes = own_t.shape[0]
    peers = arrived.shape[0]
    return pl.pallas_call(
        outer_kernel,
        grid_spec=pltpu.PrefetchScalarGridSpec(
            num_scalar_prefetch=1,
            grid=(row_blocks,),
            in_specs=[
                pl.BlockSpec((1, count, BLOCK, BLOCK), lambda g, c: (g, 0, 0, 0)),
                pl.BlockSpec(own_t.shape, lambda g, c: (0, 0)),
                pl.BlockSpec(arrived.shape, lambda g, c: (0, 0, 0)),
                pl.BlockSpec((1, BLOCK), lambda g, c: (0, g)),
                pl.BlockSpec((classes, 1), lambda g, c: (0, 0)),
            ],
            out_specs=pl.BlockSpec((classes, BLOCK), lambda g, c: (0, g)),
            scratch_shapes=[pltpu.VMEM((row_blocks + peers, classes, BLOCK), jnp.bfloat16)],
        ),
        out_shape=jax.ShapeDtypeStruct((classes, row_blocks * BLOCK), jnp.float32),
        name="outer_aggregate",
    )(tile_col, tiles, own_t, arrived, inv_row, bias_col)


def exchange(outgoing):
    return lax.all_to_all(outgoing, ("dom", "sub"), split_axis=0, concat_axis=0, tiled=True)


def on_device(
    features, w_inner, bias_inner, w_outer, bias_outer, tiles, tile_col, degrees, send_rows
):
    lists = send_rows[0]
    classes = w_outer.shape[1]
    padded = 16 * ((classes + 15) // 16)
    width = w_inner.shape[1]
    inv_sqrt = lax.rsqrt(degrees.astype(jnp.float32))
    inv_col = inv_sqrt[:, None]
    projected = (jnp.dot(features, w_inner, preferred_element_type=jnp.float32) * inv_col).astype(
        jnp.bfloat16
    )
    arrived = exchange(gather_rows(lists, projected))
    w_t = jnp.pad(w_outer.T, ((0, padded - classes), (0, 0)))
    scores_t = inner_aggregate(
        tile_col, tiles, projected.reshape(-1, BLOCK, width), arrived, inv_col, bias_inner[None, :], w_t
    )
    arrived_scores = exchange(gather_scores(lists, scores_t))
    bias_col = jnp.pad(bias_outer, (0, padded - classes))[:, None]
    logits_t = outer_aggregate(tile_col, tiles, scores_t, arrived_scores, inv_sqrt[None, :], bias_col)
    return logits_t[:classes].T


def solution(mesh):
    return jax.shard_map(
        on_device,
        mesh=mesh,
        in_specs=(
            P(("dom", "sub"), None),
            P(),
            P(),
            P(),
            P(),
            P(("dom", "sub"), None, None, None),
            P(("dom", "sub"), None),
            P(("dom", "sub")),
            P(("dom", "sub"), None, None),
        ),
        out_specs=P(("dom", "sub"), None),
        check_vma=False,
    )
```

```python
import jax
import jax.numpy as jnp
from jax import lax
from jax.experimental import pallas as pl
from jax.experimental.pallas import tpu as pltpu
from jax.sharding import PartitionSpec as P

BLOCK = 128
ROW_LISTS = 16
SCORE_LISTS = 32
QUARTER = 256
TILE_GROUPS = 4
NT = (((1,), (1,)), ((), ()))
MIB = 2**20


def whole():
    return pl.BlockSpec(memory_space=pltpu.VMEM)


def in_hbm(array):
    return pltpu.with_memory_space_constraint(array, pltpu.HBM)


def anywhere():
    return pl.BlockSpec(memory_space=pltpu.HBM)


def front_kernel(lists_ref, features_ref, w_ref, degrees_ref, sent_ref, own_ref, pick_ref):
    height = own_ref.shape[0]

    @pl.when(pl.program_id(0) == 0)
    def _():
        inv = lax.rsqrt(degrees_ref[...].astype(jnp.float32)).T
        for r in range(height // BLOCK):
            part = lax.dot_general(
                features_ref[:, r * BLOCK : (r + 1) * BLOCK],
                w_ref[...],
                (((0,), (0,)), ((), ())),
                preferred_element_type=jnp.float32,
            )
            own_ref[r * BLOCK : (r + 1) * BLOCK] = (part * inv[:, r : r + 1]).astype(jnp.bfloat16)

    by_slot = lists_ref[...].T
    row_of_lane = lax.broadcasted_iota(jnp.int32, (BLOCK, height), 1)
    for p in range(ROW_LISTS):
        pick_ref[p * BLOCK : (p + 1) * BLOCK] = (
            (by_slot[:, p : p + 1] == row_of_lane).astype(jnp.float32).astype(jnp.bfloat16)
        )
    rows = jnp.dot(pick_ref[...], own_ref[...], preferred_element_type=jnp.float32)
    sent_ref[...] = rows.astype(jnp.bfloat16).reshape(sent_ref.shape)


def front(lists, features_t, w_inner, degrees):
    peers = lists.shape[0]
    height = features_t.shape[1]
    width = w_inner.shape[1]
    return pl.pallas_call(
        front_kernel,
        grid=(peers // ROW_LISTS,),
        in_specs=[
            pl.BlockSpec((ROW_LISTS, BLOCK), lambda g: (g, 0)),
            pl.BlockSpec(features_t.shape, lambda g: (0, 0)),
            pl.BlockSpec(w_inner.shape, lambda g: (0, 0)),
            pl.BlockSpec(degrees.shape, lambda g: (0, 0)),
        ],
        out_specs=[
            pl.BlockSpec((ROW_LISTS, BLOCK, width), lambda g: (g, 0, 0)),
            pl.BlockSpec((height, width), lambda g: (0, 0)),
        ],
        out_shape=[
            jax.ShapeDtypeStruct((peers, BLOCK, width), jnp.bfloat16),
            jax.ShapeDtypeStruct((height, width), jnp.bfloat16),
        ],
        scratch_shapes=[pltpu.VMEM((ROW_LISTS * BLOCK, height), jnp.bfloat16)],
        name="front",
    )(lists, features_t, w_inner, degrees)


def fetch_tiles(tiles_ref, near_ref, sems):
    size = tiles_ref.shape[0] // TILE_GROUPS
    return [
        pltpu.make_async_copy(
            tiles_ref.at[pl.ds(g * size, size)], near_ref.at[pl.ds(g * size, size)], sems.at[g]
        )
        for g in range(TILE_GROUPS)
    ]


def inner_kernel(
    cols_ref, tiles_ref, own_ref, arrived_ref, degrees_ref, bias_ref, w_ref, out_ref, space, near, space_sems, tile_sems
):
    row_blocks, count = tiles_ref.shape[:2]
    own_blocks, peers = own_ref.shape[0], arrived_ref.shape[0]
    classes = out_ref.shape[0] // (row_blocks * BLOCK // QUARTER)
    copies = [
        pltpu.make_async_copy(arrived_ref, space.at[pl.ds(own_blocks, peers)], space_sems.at[0]),
        pltpu.make_async_copy(own_ref, space.at[pl.ds(0, own_blocks)], space_sems.at[1]),
    ]
    tile_copies = fetch_tiles(tiles_ref, near, tile_sems)
    for copy in copies:
        copy.start()
    tile_copies[0].start()
    inv = lax.rsqrt(degrees_ref[...].astype(jnp.float32)).T
    for copy in copies:
        copy.wait()
    for copy in tile_copies[1:]:
        copy.start()
    for r in range(row_blocks):
        if r % (row_blocks // TILE_GROUPS) == 0:
            tile_copies[r // (row_blocks // TILE_GROUPS)].wait()
        left = jnp.concatenate([near[r, t] for t in range(count)], axis=1)
        right = jnp.concatenate([space[cols_ref[r, t]] for t in range(count)], axis=0)
        total = jnp.dot(left, right, preferred_element_type=jnp.float32)
        scale = inv[:, r : r + 1]
        hidden = (scale * jnp.maximum(scale * total + bias_ref[...], 0.0)).astype(jnp.bfloat16)
        scores = lax.dot_general(w_ref[...], hidden, NT, preferred_element_type=jnp.float32)
        quarter, side = divmod(r * BLOCK, QUARTER)
        out_ref[quarter * classes : (quarter + 1) * classes, side : side + BLOCK] = scores.astype(jnp.bfloat16)


def inner_aggregate(tile_col, tiles, own, arrived, degrees, bias, w_t):
    row_blocks = tiles.shape[0]
    return pl.pallas_call(
        inner_kernel,
        in_specs=[pl.BlockSpec(memory_space=pltpu.SMEM)] + [anywhere()] * 3 + [whole()] * 3,
        out_specs=whole(),
        out_shape=jax.ShapeDtypeStruct((w_t.shape[0] * row_blocks * BLOCK // QUARTER, QUARTER), jnp.bfloat16),
        scratch_shapes=[
            pltpu.VMEM((own.shape[0] + arrived.shape[0],) + own.shape[1:], jnp.bfloat16),
            pltpu.VMEM(tiles.shape, jnp.bfloat16),
            pltpu.SemaphoreType.DMA((2,)),
            pltpu.SemaphoreType.DMA((TILE_GROUPS,)),
        ],
        compiler_params=pltpu.CompilerParams(vmem_limit_bytes=32 * MIB),
        name="inner_aggregate",
    )(tile_col, in_hbm(tiles), own, arrived, degrees, bias, w_t)


def gather_scores_kernel(lists_ref, stacked_ref, out_ref):
    classes = out_ref.shape[1]
    stacked = stacked_ref[...]
    group = 8
    row_of_sublane = lax.broadcasted_iota(jnp.int32, (QUARTER, group * BLOCK), 0)
    for p in range(0, SCORE_LISTS, group):
        index = jnp.concatenate([lists_ref[p + k : p + k + 1] for k in range(group)], axis=1)
        low = jnp.bitwise_and(index, QUARTER - 1)
        quarter = jnp.right_shift(index, QUARTER.bit_length() - 1)
        pick = (low == row_of_sublane).astype(jnp.float32).astype(jnp.bfloat16)
        every = jnp.dot(stacked, pick, preferred_element_type=jnp.float32)
        chosen = jnp.zeros((classes, group * BLOCK), jnp.float32)
        for q in range(stacked_ref.shape[0] // classes):
            chosen = jnp.where(quarter == q, every[q * classes : (q + 1) * classes], chosen)
        chosen = chosen.astype(jnp.bfloat16)
        for k in range(group):
            out_ref[p + k] = chosen[:, k * BLOCK : (k + 1) * BLOCK]


def gather_scores(lists, stacked, classes):
    peers = lists.shape[0]
    return pl.pallas_call(
        gather_scores_kernel,
        grid=(peers // SCORE_LISTS,),
        in_specs=[
            pl.BlockSpec((SCORE_LISTS, BLOCK), lambda g: (g, 0)),
            pl.BlockSpec(stacked.shape, lambda g: (0, 0)),
        ],
        out_specs=pl.BlockSpec((SCORE_LISTS, classes, BLOCK), lambda g: (g, 0, 0)),
        out_shape=pltpu.HBM((peers, classes, BLOCK), jnp.bfloat16),
        compiler_params=pltpu.CompilerParams(vmem_limit_bytes=16 * MIB),
        name="gather_scores",
    )(lists, stacked)


def outer_kernel(cols_ref, tiles_ref, stacked_ref, arrived_ref, degrees_ref, bias_ref, out_ref, space, near, tile_sems):
    row_blocks, count = tiles_ref.shape[:2]
    padded = arrived_ref.shape[1]
    classes = out_ref.shape[0]
    tile_copies = fetch_tiles(tiles_ref, near, tile_sems)
    for copy in tile_copies:
        copy.start()
    for r in range(row_blocks):
        quarter, side = divmod(r * BLOCK, QUARTER)
        space[r] = stacked_ref[quarter * padded : (quarter + 1) * padded, side : side + BLOCK]
    space[row_blocks:] = arrived_ref[...]
    inv = lax.rsqrt(degrees_ref[...].astype(jnp.float32))
    bias = bias_ref[...].T
    for r in range(row_blocks):
        if r % (row_blocks // TILE_GROUPS) == 0:
            tile_copies[r // (row_blocks // TILE_GROUPS)].wait()
        left = jnp.concatenate([near[r, t] for t in range(count)], axis=1)
        right = jnp.concatenate([space[cols_ref[r, t]] for t in range(count)], axis=1)
        total = lax.dot_general(left, right, NT, preferred_element_type=jnp.float32).T
        out_ref[:, r * BLOCK : (r + 1) * BLOCK] = inv[r : r + 1] * total[:classes] + bias


def outer_aggregate(tile_col, tiles, stacked, arrived, degrees, bias):
    row_blocks = tiles.shape[0]
    peers, padded, _ = arrived.shape
    return pl.pallas_call(
        outer_kernel,
        in_specs=[pl.BlockSpec(memory_space=pltpu.SMEM), anywhere()] + [whole()] * 4,
        out_specs=whole(),
        out_shape=jax.ShapeDtypeStruct((bias.shape[1], row_blocks * BLOCK), jnp.float32),
        scratch_shapes=[
            pltpu.VMEM((row_blocks + peers, padded, BLOCK), jnp.bfloat16),
            pltpu.VMEM(tiles.shape, jnp.bfloat16),
            pltpu.SemaphoreType.DMA((TILE_GROUPS,)),
        ],
        compiler_params=pltpu.CompilerParams(vmem_limit_bytes=24 * MIB),
        name="outer_aggregate",
    )(tile_col, in_hbm(tiles), stacked, arrived, degrees, bias)


def exchange(outgoing):
    return lax.all_to_all(outgoing, ("dom", "sub"), split_axis=0, concat_axis=0, tiled=True)


def on_device(
    features, w_inner, bias_inner, w_outer, bias_outer, tiles, tile_col, degrees, send_rows
):
    lists = send_rows[0]
    classes = w_outer.shape[1]
    padded = 16 * ((classes + 15) // 16)
    width = w_inner.shape[1]
    degree_rows = degrees.reshape(-1, BLOCK)
    outgoing, own = front(lists, features.T, w_inner, degree_rows)
    arrived = exchange(outgoing)
    w_t = jnp.pad(w_outer.T, ((0, padded - classes), (0, 0)))
    stacked = inner_aggregate(
        tile_col, tiles, own.reshape(-1, BLOCK, width), arrived, degree_rows, bias_inner[None, :], w_t
    )
    arrived_scores = exchange(gather_scores(lists, stacked, padded))
    logits_t = outer_aggregate(
        tile_col, tiles, stacked, arrived_scores, degree_rows, bias_outer[None, :]
    )
    return logits_t.T


def solution(mesh):
    return jax.shard_map(
        on_device,
        mesh=mesh,
        in_specs=(
            P(("dom", "sub"), None),
            P(),
            P(),
            P(),
            P(),
            P(("dom", "sub"), None, None, None),
            P(("dom", "sub"), None),
            P(("dom", "sub")),
            P(("dom", "sub"), None, None),
        ),
        out_specs=P(("dom", "sub"), None),
        check_vma=False,
    )
```

```python
import jax
import jax.numpy as jnp
from jax import lax
from jax.experimental import pallas as pl
from jax.experimental.pallas import tpu as pltpu
from jax.sharding import PartitionSpec as P

BLOCK = 128
ROW_LISTS = 32
SCORE_LISTS = 8
QUARTER = 256
TILE_GROUPS = 4
SENDS = 4
NT = (((1,), (1,)), ((), ()))
MIB = 2**20


def whole():
    return pl.BlockSpec(memory_space=pltpu.VMEM)


def in_hbm(array):
    return pltpu.with_memory_space_constraint(array, pltpu.HBM)


def anywhere():
    return pl.BlockSpec(memory_space=pltpu.HBM)


def front_kernel(lists_ref, features_ref, w_ref, degrees_ref, sent_ref, own_ref, pick_ref):
    height = own_ref.shape[0]

    @pl.when(pl.program_id(0) == 0)
    def _():
        inv = lax.rsqrt(degrees_ref[...].astype(jnp.float32)).T
        for r in range(height // BLOCK):
            part = lax.dot_general(
                features_ref[:, r * BLOCK : (r + 1) * BLOCK],
                w_ref[...],
                (((0,), (0,)), ((), ())),
                preferred_element_type=jnp.float32,
            )
            own_ref[r * BLOCK : (r + 1) * BLOCK] = (part * inv[:, r : r + 1]).astype(jnp.bfloat16)

    by_slot = lists_ref[...].T
    row_of_lane = lax.broadcasted_iota(jnp.int32, (BLOCK, height), 1)
    for p in range(ROW_LISTS):
        pick_ref[p * BLOCK : (p + 1) * BLOCK] = (
            (by_slot[:, p : p + 1] == row_of_lane).astype(jnp.float32).astype(jnp.bfloat16)
        )
    rows = jnp.dot(pick_ref[...], own_ref[...], preferred_element_type=jnp.float32)
    sent_ref[...] = rows.astype(jnp.bfloat16).reshape(sent_ref.shape)


def front(lists, features_t, w_inner, degrees):
    peers = lists.shape[0]
    height = features_t.shape[1]
    width = w_inner.shape[1]
    return pl.pallas_call(
        front_kernel,
        grid=(peers // ROW_LISTS,),
        in_specs=[
            pl.BlockSpec((ROW_LISTS, BLOCK), lambda g: (g, 0)),
            pl.BlockSpec(features_t.shape, lambda g: (0, 0)),
            pl.BlockSpec(w_inner.shape, lambda g: (0, 0)),
            pl.BlockSpec(degrees.shape, lambda g: (0, 0)),
        ],
        out_specs=[
            pl.BlockSpec((ROW_LISTS, BLOCK, width), lambda g: (g, 0, 0)),
            pl.BlockSpec((height, width), lambda g: (0, 0)),
        ],
        out_shape=[
            jax.ShapeDtypeStruct((peers, BLOCK, width), jnp.bfloat16),
            jax.ShapeDtypeStruct((height, width), jnp.bfloat16),
        ],
        scratch_shapes=[pltpu.VMEM((ROW_LISTS * BLOCK, height), jnp.bfloat16)],
        name="front",
    )(lists, features_t, w_inner, degrees)


def fetch_tiles(tiles_ref, near_ref, sems):
    size = tiles_ref.shape[0] // TILE_GROUPS
    return [
        pltpu.make_async_copy(
            tiles_ref.at[pl.ds(g * size, size)], near_ref.at[pl.ds(g * size, size)], sems.at[g]
        )
        for g in range(TILE_GROUPS)
    ]


def inner_kernel(
    cols_ref,
    lists_ref,
    tiles_ref,
    own_ref,
    arrived_ref,
    degrees_ref,
    bias_ref,
    w_ref,
    stacked_ref,
    sent_ref,
    space,
    near,
    picks,
    hidden,
    outgoing,
    space_sems,
    tile_sems,
    sent_sems,
):
    row_blocks, count = tiles_ref.shape[:2]
    own_blocks, peers = own_ref.shape[0], arrived_ref.shape[0]
    padded = outgoing.shape[1]
    classes = w_ref.shape[0]
    quarters = stacked_ref.shape[0] // padded
    steps = peers // SCORE_LISTS
    copies = [
        pltpu.make_async_copy(arrived_ref, space.at[pl.ds(own_blocks, peers)], space_sems.at[0]),
        pltpu.make_async_copy(own_ref, space.at[pl.ds(0, own_blocks)], space_sems.at[1]),
    ]
    tile_copies = fetch_tiles(tiles_ref, near, tile_sems)
    for copy in copies:
        copy.start()
    tile_copies[0].start()

    def list_row(g):
        rows = lists_ref[g * SCORE_LISTS : (g + 1) * SCORE_LISTS]
        return jnp.concatenate([rows[k : k + 1] for k in range(SCORE_LISTS)], axis=1)

    row_of_sublane = lax.broadcasted_iota(jnp.int32, (QUARTER, SCORE_LISTS * BLOCK), 0)
    for g in range(steps):
        low = jnp.bitwise_and(list_row(g), QUARTER - 1)
        picks[g] = (low == row_of_sublane).astype(jnp.float32).astype(jnp.bfloat16)

    inv = lax.rsqrt(degrees_ref[...].astype(jnp.float32)).T
    for copy in copies:
        copy.wait()
    for copy in tile_copies[1:]:
        copy.start()
    for r in range(row_blocks):
        if r % (row_blocks // TILE_GROUPS) == 0:
            tile_copies[r // (row_blocks // TILE_GROUPS)].wait()
        left = jnp.concatenate([near[r, t] for t in range(count)], axis=1)
        right = jnp.concatenate([space[cols_ref[r, t]] for t in range(count)], axis=0)
        total = jnp.dot(left, right, preferred_element_type=jnp.float32)
        scale = inv[:, r : r + 1]
        row = scale * jnp.maximum(scale * total + bias_ref[...], 0.0)
        hidden[r * BLOCK : (r + 1) * BLOCK] = row.astype(jnp.bfloat16)

    scores = lax.dot_general(w_ref[...], hidden[...], NT, preferred_element_type=jnp.float32)
    scores = jnp.concatenate([scores, jnp.zeros((padded - classes, scores.shape[1]), jnp.float32)], axis=0)
    scores = scores.astype(jnp.bfloat16)
    for q in range(quarters):
        stacked_ref[q * padded : (q + 1) * padded] = scores[:, q * QUARTER : (q + 1) * QUARTER]

    sends = []
    per_send = steps // SENDS
    for g in range(steps):
        quarter = jnp.right_shift(list_row(g), QUARTER.bit_length() - 1)
        every = jnp.dot(stacked_ref[...], picks[g], preferred_element_type=jnp.float32)
        chosen = jnp.zeros((padded, SCORE_LISTS * BLOCK), jnp.float32)
        for q in range(quarters):
            chosen = jnp.where(quarter == q, every[q * padded : (q + 1) * padded], chosen)
        chosen = chosen.astype(jnp.bfloat16)
        for k in range(SCORE_LISTS):
            outgoing[g * SCORE_LISTS + k] = chosen[:, k * BLOCK : (k + 1) * BLOCK]
        if (g + 1) % per_send == 0:
            first = (g + 1 - per_send) * SCORE_LISTS
            part = pl.ds(first, per_send * SCORE_LISTS)
            send = pltpu.make_async_copy(outgoing.at[part], sent_ref.at[part], sent_sems.at[g // per_send])
            send.start()
            sends.append(send)
    for send in sends:
        send.wait()


def inner_aggregate(tile_col, lists, tiles, own, arrived, degrees, bias, w_t, padded):
    row_blocks = tiles.shape[0]
    peers, _, width = arrived.shape
    height = row_blocks * BLOCK
    return pl.pallas_call(
        inner_kernel,
        in_specs=[pl.BlockSpec(memory_space=pltpu.SMEM), whole()] + [anywhere()] * 3 + [whole()] * 3,
        out_specs=[whole(), anywhere()],
        out_shape=[
            jax.ShapeDtypeStruct((padded * height // QUARTER, QUARTER), jnp.bfloat16),
            pltpu.HBM((peers, padded, BLOCK), jnp.bfloat16),
        ],
        scratch_shapes=[
            pltpu.VMEM((own.shape[0] + peers, BLOCK, width), jnp.bfloat16),
            pltpu.VMEM(tiles.shape, jnp.bfloat16),
            pltpu.VMEM((peers // SCORE_LISTS, QUARTER, SCORE_LISTS * BLOCK), jnp.bfloat16),
            pltpu.VMEM((height, width), jnp.bfloat16),
            pltpu.VMEM((peers, padded, BLOCK), jnp.bfloat16),
            pltpu.SemaphoreType.DMA((2,)),
            pltpu.SemaphoreType.DMA((TILE_GROUPS,)),
            pltpu.SemaphoreType.DMA((SENDS,)),
        ],
        compiler_params=pltpu.CompilerParams(vmem_limit_bytes=44 * MIB),
        name="inner_aggregate",
    )(tile_col, lists, in_hbm(tiles), own, in_hbm(arrived), degrees, bias, w_t)


def outer_kernel(cols_ref, tiles_ref, stacked_ref, arrived_ref, degrees_ref, bias_ref, out_ref, space, near, tile_sems):
    row_blocks, count = tiles_ref.shape[:2]
    padded = arrived_ref.shape[1]
    classes = out_ref.shape[0]
    tile_copies = fetch_tiles(tiles_ref, near, tile_sems)
    for copy in tile_copies:
        copy.start()
    for r in range(row_blocks):
        quarter, side = divmod(r * BLOCK, QUARTER)
        space[r] = stacked_ref[quarter * padded : (quarter + 1) * padded, side : side + BLOCK]
    space[row_blocks:] = arrived_ref[...]
    inv = lax.rsqrt(degrees_ref[...].astype(jnp.float32))
    bias = bias_ref[...].T
    for r in range(row_blocks):
        if r % (row_blocks // TILE_GROUPS) == 0:
            tile_copies[r // (row_blocks // TILE_GROUPS)].wait()
        left = jnp.concatenate([near[r, t] for t in range(count)], axis=1)
        right = jnp.concatenate([space[cols_ref[r, t]] for t in range(count)], axis=1)
        total = lax.dot_general(left, right, NT, preferred_element_type=jnp.float32).T
        out_ref[:, r * BLOCK : (r + 1) * BLOCK] = inv[r : r + 1] * total[:classes] + bias


def outer_aggregate(tile_col, tiles, stacked, arrived, degrees, bias):
    row_blocks = tiles.shape[0]
    peers, padded, _ = arrived.shape
    return pl.pallas_call(
        outer_kernel,
        in_specs=[pl.BlockSpec(memory_space=pltpu.SMEM), anywhere()] + [whole()] * 4,
        out_specs=whole(),
        out_shape=jax.ShapeDtypeStruct((bias.shape[1], row_blocks * BLOCK), jnp.float32),
        scratch_shapes=[
            pltpu.VMEM((row_blocks + peers, padded, BLOCK), jnp.bfloat16),
            pltpu.VMEM(tiles.shape, jnp.bfloat16),
            pltpu.SemaphoreType.DMA((TILE_GROUPS,)),
        ],
        compiler_params=pltpu.CompilerParams(vmem_limit_bytes=24 * MIB),
        name="outer_aggregate",
    )(tile_col, in_hbm(tiles), stacked, arrived, degrees, bias)


def exchange(outgoing):
    return lax.all_to_all(outgoing, ("dom", "sub"), split_axis=0, concat_axis=0, tiled=True)


def on_device(
    features, w_inner, bias_inner, w_outer, bias_outer, tiles, tile_col, degrees, send_rows
):
    lists = send_rows[0]
    classes = w_outer.shape[1]
    padded = 16 * ((classes + 15) // 16)
    width = w_inner.shape[1]
    degree_rows = degrees.reshape(-1, BLOCK)
    outgoing, own = front(lists, features.T, w_inner, degree_rows)
    arrived = exchange(outgoing)
    stacked, outgoing_scores = inner_aggregate(
        tile_col,
        lists,
        tiles,
        own.reshape(-1, BLOCK, width),
        arrived,
        degree_rows,
        bias_inner[None, :],
        w_outer.T,
        padded,
    )
    arrived_scores = exchange(outgoing_scores)
    logits_t = outer_aggregate(
        tile_col, tiles, stacked, arrived_scores, degree_rows, bias_outer[None, :]
    )
    return logits_t.T


def solution(mesh):
    return jax.shard_map(
        on_device,
        mesh=mesh,
        in_specs=(
            P(("dom", "sub"), None),
            P(),
            P(),
            P(),
            P(),
            P(("dom", "sub"), None, None, None),
            P(("dom", "sub"), None),
            P(("dom", "sub")),
            P(("dom", "sub"), None, None),
        ),
        out_specs=P(("dom", "sub"), None),
        check_vma=False,
    )
```

```python
import jax
import jax.numpy as jnp
from jax import lax
from jax.experimental import pallas as pl
from jax.experimental.pallas import tpu as pltpu
from jax.sharding import PartitionSpec as P

BLOCK = 128
ROW_LISTS = 32
SCORE_LISTS = 8
QUARTER = 256
SCORE_UNROLL = 4
NT = (((1,), (1,)), ((), ()))
MIB = 2**20


def whole():
    return pl.BlockSpec(memory_space=pltpu.VMEM)


def in_hbm(array):
    return pltpu.with_memory_space_constraint(array, pltpu.HBM)


def in_vmem(array):
    return pltpu.with_memory_space_constraint(array, pltpu.VMEM)


def anywhere():
    return pl.BlockSpec(memory_space=pltpu.HBM)


def front_kernel(
    lists_ref, features_ref, w_ref, degrees_ref, tiles_ref, sent_ref, own_ref, near_ref, pick_ref, tile_sem
):
    height = own_ref.shape[0]
    fetch = pltpu.make_async_copy(tiles_ref, near_ref, tile_sem.at[0])

    @pl.when(pl.program_id(0) == 0)
    def _():
        fetch.start()
        inv = lax.rsqrt(degrees_ref[...].astype(jnp.float32)).T
        for r in range(height // BLOCK):
            part = lax.dot_general(
                features_ref[:, r * BLOCK : (r + 1) * BLOCK],
                w_ref[...],
                (((0,), (0,)), ((), ())),
                preferred_element_type=jnp.float32,
            )
            own_ref[r * BLOCK : (r + 1) * BLOCK] = (part * inv[:, r : r + 1]).astype(jnp.bfloat16)

    by_slot = lists_ref[...].T
    row_of_lane = lax.broadcasted_iota(jnp.int32, (BLOCK, height), 1)
    for p in range(ROW_LISTS):
        pick_ref[p * BLOCK : (p + 1) * BLOCK] = (
            (by_slot[:, p : p + 1] == row_of_lane).astype(jnp.float32).astype(jnp.bfloat16)
        )
    rows = jnp.dot(pick_ref[...], own_ref[...], preferred_element_type=jnp.float32)
    sent_ref[...] = rows.astype(jnp.bfloat16).reshape(sent_ref.shape)

    @pl.when(pl.program_id(0) == pl.num_programs(0) - 1)
    def _():
        fetch.wait()


def front(lists, features_t, w_inner, degrees, tiles):
    peers = lists.shape[0]
    height = features_t.shape[1]
    width = w_inner.shape[1]
    return pl.pallas_call(
        front_kernel,
        grid=(peers // ROW_LISTS,),
        in_specs=[
            pl.BlockSpec((ROW_LISTS, BLOCK), lambda g: (g, 0)),
            pl.BlockSpec(features_t.shape, lambda g: (0, 0)),
            pl.BlockSpec(w_inner.shape, lambda g: (0, 0)),
            pl.BlockSpec(degrees.shape, lambda g: (0, 0)),
            pl.BlockSpec(memory_space=pl.ANY),
        ],
        out_specs=[
            pl.BlockSpec((ROW_LISTS, BLOCK, width), lambda g: (g, 0, 0)),
            pl.BlockSpec((height, width), lambda g: (0, 0)),
            pl.BlockSpec(memory_space=pl.ANY),
        ],
        out_shape=[
            pltpu.HBM((peers, BLOCK, width), jnp.bfloat16),
            jax.ShapeDtypeStruct((height, width), jnp.bfloat16),
            pltpu.VMEM(tiles.shape, tiles.dtype),
        ],
        scratch_shapes=[
            pltpu.VMEM((ROW_LISTS * BLOCK, height), jnp.bfloat16),
            pltpu.SemaphoreType.DMA((1,)),
        ],
        compiler_params=pltpu.CompilerParams(vmem_limit_bytes=28 * MIB),
        name="front",
    )(in_hbm(lists), in_hbm(features_t), in_hbm(w_inner), in_hbm(degrees), in_hbm(tiles))


def inner_kernel(
    cols_ref,
    lists_ref,
    tiles_ref,
    own_ref,
    arrived_ref,
    degrees_ref,
    bias_ref,
    w_ref,
    stacked_ref,
    sent_ref,
    hidden,
    outgoing,
    sent_sems,
):
    row_blocks, count = tiles_ref.shape[:2]
    own_blocks, peers = own_ref.shape[0], arrived_ref.shape[0]
    padded = outgoing.shape[1]
    classes = w_ref.shape[0]
    quarters = stacked_ref.shape[0] // padded
    steps = peers // SCORE_LISTS

    def block(c):
        near = own_ref[jnp.minimum(c, own_blocks - 1)]
        far = arrived_ref[jnp.maximum(c - own_blocks, 0)]
        return jnp.where(c < own_blocks, near, far)

    def list_row(g):
        rows = lists_ref[pl.ds(pl.multiple_of(g * SCORE_LISTS, SCORE_LISTS), SCORE_LISTS)]
        return jnp.concatenate([rows[k : k + 1] for k in range(SCORE_LISTS)], axis=1)

    row_of_sublane = lax.broadcasted_iota(jnp.int32, (QUARTER, SCORE_LISTS * BLOCK), 0)

    inv = lax.rsqrt(degrees_ref[...].astype(jnp.float32)).T
    for r in range(row_blocks):
        left = jnp.concatenate([tiles_ref[r, t] for t in range(count)], axis=1)
        right = jnp.concatenate([block(cols_ref[r, t]) for t in range(count)], axis=0)
        total = jnp.dot(left, right, preferred_element_type=jnp.float32)
        scale = inv[:, r : r + 1]
        row = scale * jnp.maximum(scale * total + bias_ref[...], 0.0)
        hidden[r * BLOCK : (r + 1) * BLOCK] = row.astype(jnp.bfloat16)

    scores = lax.dot_general(w_ref[...], hidden[...], NT, preferred_element_type=jnp.float32)
    scores = jnp.concatenate([scores, jnp.zeros((padded - classes, scores.shape[1]), jnp.float32)], axis=0)
    scores = scores.astype(jnp.bfloat16)
    for q in range(quarters):
        stacked_ref[q * padded : (q + 1) * padded] = scores[:, q * QUARTER : (q + 1) * QUARTER]

    def send(h):
        part = pl.ds(h * SCORE_UNROLL * SCORE_LISTS, SCORE_UNROLL * SCORE_LISTS)
        return pltpu.make_async_copy(outgoing.at[part], sent_ref.at[part], sent_sems.at[h])

    @pl.loop(0, steps // SCORE_UNROLL)
    def _(h):
        for u in range(SCORE_UNROLL):
            g = h * SCORE_UNROLL + u
            quarter = jnp.right_shift(list_row(g), QUARTER.bit_length() - 1)
            low = jnp.bitwise_and(list_row(g), QUARTER - 1)
            pick = (low == row_of_sublane).astype(jnp.float32).astype(jnp.bfloat16)
            every = jnp.dot(stacked_ref[...], pick, preferred_element_type=jnp.float32)
            chosen = jnp.zeros((padded, SCORE_LISTS * BLOCK), jnp.float32)
            for q in range(quarters):
                chosen = jnp.where(quarter == q, every[q * padded : (q + 1) * padded], chosen)
            chosen = chosen.astype(jnp.bfloat16)
            for k in range(SCORE_LISTS):
                outgoing[g * SCORE_LISTS + k] = chosen[:, k * BLOCK : (k + 1) * BLOCK]
        send(h).start()

    for h in range(steps // SCORE_UNROLL):
        send(h).wait()


def inner_aggregate(tile_col, lists, near_tiles, own, arrived, degrees, bias, w_t, padded):
    row_blocks = near_tiles.shape[0]
    peers, _, width = arrived.shape
    height = row_blocks * BLOCK
    return pl.pallas_call(
        inner_kernel,
        in_specs=[pl.BlockSpec(memory_space=pltpu.SMEM), whole()] + [whole()] * 6,
        out_specs=[whole(), anywhere()],
        out_shape=[
            jax.ShapeDtypeStruct((padded * height // QUARTER, QUARTER), jnp.bfloat16),
            pltpu.HBM((peers, padded, BLOCK), jnp.bfloat16),
        ],
        scratch_shapes=[
            pltpu.VMEM((height, width), jnp.bfloat16),
            pltpu.VMEM((peers, padded, BLOCK), jnp.bfloat16),
            pltpu.SemaphoreType.DMA((peers // SCORE_LISTS // SCORE_UNROLL,)),
        ],
        compiler_params=pltpu.CompilerParams(vmem_limit_bytes=20 * MIB),
        name="inner_aggregate",
    )(tile_col, lists, in_vmem(near_tiles), own, in_vmem(arrived), degrees, bias, w_t)


def outer_kernel(cols_ref, tiles_ref, stacked_ref, arrived_ref, degrees_ref, bias_ref, out_ref, space):
    row_blocks, count = tiles_ref.shape[:2]
    padded = arrived_ref.shape[1]
    classes = out_ref.shape[0]
    for r in range(row_blocks):
        quarter, side = divmod(r * BLOCK, QUARTER)
        space[r] = stacked_ref[quarter * padded : (quarter + 1) * padded, side : side + BLOCK]
    space[row_blocks:] = arrived_ref[...]
    inv = lax.rsqrt(degrees_ref[...].astype(jnp.float32))
    bias = bias_ref[...].T
    for r in range(row_blocks):
        left = jnp.concatenate([tiles_ref[r, t] for t in range(count)], axis=1)
        right = jnp.concatenate([space[cols_ref[r, t]] for t in range(count)], axis=1)
        total = lax.dot_general(left, right, NT, preferred_element_type=jnp.float32).T
        out_ref[:, r * BLOCK : (r + 1) * BLOCK] = inv[r : r + 1] * total[:classes] + bias


def outer_aggregate(tile_col, near_tiles, stacked, arrived, degrees, bias):
    row_blocks = near_tiles.shape[0]
    peers, padded, _ = arrived.shape
    return pl.pallas_call(
        outer_kernel,
        in_specs=[pl.BlockSpec(memory_space=pltpu.SMEM)] + [whole()] * 5,
        out_specs=whole(),
        out_shape=jax.ShapeDtypeStruct((bias.shape[1], row_blocks * BLOCK), jnp.float32),
        scratch_shapes=[pltpu.VMEM((row_blocks + peers, padded, BLOCK), jnp.bfloat16)],
        compiler_params=pltpu.CompilerParams(vmem_limit_bytes=16 * MIB),
        name="outer_aggregate",
    )(tile_col, in_vmem(near_tiles), stacked, arrived, degrees, bias)


def exchange(outgoing):
    return lax.all_to_all(outgoing, ("dom", "sub"), split_axis=0, concat_axis=0, tiled=True)


def on_device(
    features, w_inner, bias_inner, w_outer, bias_outer, tiles, tile_col, degrees, send_rows
):
    lists = send_rows[0]
    classes = w_outer.shape[1]
    padded = 16 * ((classes + 15) // 16)
    width = w_inner.shape[1]
    degree_rows = degrees.reshape(-1, BLOCK)
    outgoing, own, near_tiles = front(lists, features.T, w_inner, degree_rows, tiles)
    arrived = exchange(outgoing)
    stacked, outgoing_scores = inner_aggregate(
        tile_col,
        lists,
        near_tiles,
        own.reshape(-1, BLOCK, width),
        arrived,
        degree_rows,
        bias_inner[None, :],
        w_outer.T,
        padded,
    )
    arrived_scores = exchange(outgoing_scores)
    logits_t = outer_aggregate(
        tile_col, near_tiles, stacked, arrived_scores, degree_rows, bias_outer[None, :]
    )
    return logits_t.T


def solution(mesh):
    return jax.shard_map(
        on_device,
        mesh=mesh,
        in_specs=(
            P(("dom", "sub"), None),
            P(),
            P(),
            P(),
            P(),
            P(("dom", "sub"), None, None, None),
            P(("dom", "sub"), None),
            P(("dom", "sub")),
            P(("dom", "sub"), None, None),
        ),
        out_specs=P(("dom", "sub"), None),
        check_vma=False,
    )
```

```python
import jax
import jax.numpy as jnp
from jax import lax
from jax.experimental import pallas as pl
from jax.experimental.pallas import tpu as pltpu
from jax.sharding import PartitionSpec as P

BLOCK = 128
ROW_LISTS = 32
SCORE_LISTS = 8
QUARTER = 256
SCORE_UNROLL = 4
NT = (((1,), (1,)), ((), ()))
MIB = 2**20


def whole():
    return pl.BlockSpec(memory_space=pltpu.VMEM)


def in_hbm(array):
    return pltpu.with_memory_space_constraint(array, pltpu.HBM)


def in_vmem(array):
    return pltpu.with_memory_space_constraint(array, pltpu.VMEM)


def anywhere():
    return pl.BlockSpec(memory_space=pltpu.HBM)


def front_kernel(
    lists_ref, features_ref, w_ref, degrees_ref, tiles_ref, sent_ref, own_ref, near_ref, pick_ref, tile_sem
):
    height = own_ref.shape[0]
    fetch = pltpu.make_async_copy(tiles_ref, near_ref, tile_sem.at[0])

    @pl.when(pl.program_id(0) == 0)
    def _():
        fetch.start()
        inv = lax.rsqrt(degrees_ref[...].astype(jnp.float32)).T
        for r in range(height // BLOCK):
            part = lax.dot_general(
                features_ref[:, r * BLOCK : (r + 1) * BLOCK],
                w_ref[...],
                (((0,), (0,)), ((), ())),
                preferred_element_type=jnp.float32,
            )
            own_ref[r * BLOCK : (r + 1) * BLOCK] = (part * inv[:, r : r + 1]).astype(jnp.bfloat16)

    by_slot = lists_ref[...].T
    row_of_lane = lax.broadcasted_iota(jnp.int32, (BLOCK, height), 1)
    for p in range(ROW_LISTS):
        pick_ref[p * BLOCK : (p + 1) * BLOCK] = (
            (by_slot[:, p : p + 1] == row_of_lane).astype(jnp.float32).astype(jnp.bfloat16)
        )
    rows = jnp.dot(pick_ref[...], own_ref[...], preferred_element_type=jnp.float32)
    sent_ref[...] = rows.astype(jnp.bfloat16).reshape(sent_ref.shape)

    @pl.when(pl.program_id(0) == pl.num_programs(0) - 1)
    def _():
        fetch.wait()


def front(lists, features_t, w_inner, degrees, tiles):
    peers = lists.shape[0]
    height = features_t.shape[1]
    width = w_inner.shape[1]
    return pl.pallas_call(
        front_kernel,
        grid=(peers // ROW_LISTS,),
        in_specs=[
            pl.BlockSpec((ROW_LISTS, BLOCK), lambda g: (g, 0)),
            pl.BlockSpec(features_t.shape, lambda g: (0, 0)),
            pl.BlockSpec(w_inner.shape, lambda g: (0, 0)),
            pl.BlockSpec(degrees.shape, lambda g: (0, 0)),
            pl.BlockSpec(memory_space=pl.ANY),
        ],
        out_specs=[
            pl.BlockSpec((ROW_LISTS, BLOCK, width), lambda g: (g, 0, 0)),
            pl.BlockSpec((height, width), lambda g: (0, 0)),
            pl.BlockSpec(memory_space=pl.ANY),
        ],
        out_shape=[
            pltpu.HBM((peers, BLOCK, width), jnp.bfloat16),
            jax.ShapeDtypeStruct((height, width), jnp.bfloat16),
            pltpu.VMEM(tiles.shape, tiles.dtype),
        ],
        scratch_shapes=[
            pltpu.VMEM((ROW_LISTS * BLOCK, height), jnp.bfloat16),
            pltpu.SemaphoreType.DMA((1,)),
        ],
        compiler_params=pltpu.CompilerParams(vmem_limit_bytes=28 * MIB),
        name="front",
    )(in_hbm(lists), in_hbm(features_t), in_hbm(w_inner), in_hbm(degrees), in_hbm(tiles))


def inner_kernel(
    cols_ref,
    lists_ref,
    tiles_ref,
    own_ref,
    arrived_ref,
    degrees_ref,
    bias_ref,
    w_ref,
    stacked_ref,
    sent_ref,
    hidden,
    outgoing,
    sent_sems,
):
    row_blocks, count = tiles_ref.shape[:2]
    own_blocks, peers = own_ref.shape[0], arrived_ref.shape[0]
    padded = outgoing.shape[1]
    classes = w_ref.shape[0]
    quarters = stacked_ref.shape[0] // padded
    steps = peers // SCORE_LISTS

    def block(c):
        near = own_ref[jnp.minimum(c, own_blocks - 1)]
        far = arrived_ref[jnp.maximum(c - own_blocks, 0)]
        return jnp.where(c < own_blocks, near, far)

    def list_row(g):
        rows = lists_ref[pl.ds(pl.multiple_of(g * SCORE_LISTS, SCORE_LISTS), SCORE_LISTS)]
        return jnp.concatenate([rows[k : k + 1] for k in range(SCORE_LISTS)], axis=1)

    row_of_sublane = lax.broadcasted_iota(jnp.int16, (QUARTER, SCORE_LISTS * BLOCK), 0)
    one = jnp.ones(row_of_sublane.shape, jnp.bfloat16)
    zero = jnp.zeros(row_of_sublane.shape, jnp.bfloat16)

    inv = lax.rsqrt(degrees_ref[...].astype(jnp.float32)).T
    for r in range(row_blocks):
        left = jnp.concatenate([tiles_ref[r, t] for t in range(count)], axis=1)
        right = jnp.concatenate([block(cols_ref[r, t]) for t in range(count)], axis=0)
        total = jnp.dot(left, right, preferred_element_type=jnp.float32)
        scale = inv[:, r : r + 1]
        row = scale * jnp.maximum(scale * total + bias_ref[...], 0.0)
        hidden[r * BLOCK : (r + 1) * BLOCK] = row.astype(jnp.bfloat16)

    scores = lax.dot_general(w_ref[...], hidden[...], NT, preferred_element_type=jnp.float32)
    scores = jnp.concatenate([scores, jnp.zeros((padded - classes, scores.shape[1]), jnp.float32)], axis=0)
    scores = scores.astype(jnp.bfloat16)
    for q in range(quarters):
        stacked_ref[q * padded : (q + 1) * padded] = scores[:, q * QUARTER : (q + 1) * QUARTER]

    def send(h):
        part = pl.ds(h * SCORE_UNROLL * SCORE_LISTS, SCORE_UNROLL * SCORE_LISTS)
        return pltpu.make_async_copy(outgoing.at[part], sent_ref.at[part], sent_sems.at[h])

    @pl.loop(0, steps // SCORE_UNROLL)
    def _(h):
        for u in range(SCORE_UNROLL):
            g = h * SCORE_UNROLL + u
            quarter = jnp.right_shift(list_row(g), QUARTER.bit_length() - 1)
            low = jnp.bitwise_and(list_row(g), QUARTER - 1)
            near_row = jnp.broadcast_to(low, row_of_sublane.shape).astype(jnp.int16) == row_of_sublane
            pick = jnp.where(near_row, one, zero)
            every = jnp.dot(stacked_ref[...], pick, preferred_element_type=jnp.float32)
            chosen = jnp.zeros((padded, SCORE_LISTS * BLOCK), jnp.float32)
            for q in range(quarters):
                chosen = jnp.where(quarter == q, every[q * padded : (q + 1) * padded], chosen)
            chosen = chosen.astype(jnp.bfloat16)
            for k in range(SCORE_LISTS):
                outgoing[g * SCORE_LISTS + k] = chosen[:, k * BLOCK : (k + 1) * BLOCK]
        send(h).start()

    for h in range(steps // SCORE_UNROLL):
        send(h).wait()


def inner_aggregate(tile_col, lists, near_tiles, own, arrived, degrees, bias, w_t, padded):
    row_blocks = near_tiles.shape[0]
    peers, _, width = arrived.shape
    height = row_blocks * BLOCK
    return pl.pallas_call(
        inner_kernel,
        in_specs=[pl.BlockSpec(memory_space=pltpu.SMEM), whole()] + [whole()] * 6,
        out_specs=[whole(), anywhere()],
        out_shape=[
            jax.ShapeDtypeStruct((padded * height // QUARTER, QUARTER), jnp.bfloat16),
            pltpu.HBM((peers, padded, BLOCK), jnp.bfloat16),
        ],
        scratch_shapes=[
            pltpu.VMEM((height, width), jnp.bfloat16),
            pltpu.VMEM((peers, padded, BLOCK), jnp.bfloat16),
            pltpu.SemaphoreType.DMA((peers // SCORE_LISTS // SCORE_UNROLL,)),
        ],
        compiler_params=pltpu.CompilerParams(vmem_limit_bytes=20 * MIB),
        name="inner_aggregate",
    )(tile_col, lists, in_vmem(near_tiles), own, in_vmem(arrived), degrees, bias, w_t)


def outer_kernel(cols_ref, tiles_ref, stacked_ref, arrived_ref, degrees_ref, bias_ref, out_ref, space):
    row_blocks, count = tiles_ref.shape[:2]
    padded = arrived_ref.shape[1]
    classes = out_ref.shape[0]
    for r in range(row_blocks):
        quarter, side = divmod(r * BLOCK, QUARTER)
        space[r] = stacked_ref[quarter * padded : (quarter + 1) * padded, side : side + BLOCK]
    space[row_blocks:] = arrived_ref[...]
    inv = lax.rsqrt(degrees_ref[...].astype(jnp.float32))
    bias = bias_ref[...].T
    for r in range(row_blocks):
        left = jnp.concatenate([tiles_ref[r, t] for t in range(count)], axis=1)
        right = jnp.concatenate([space[cols_ref[r, t]] for t in range(count)], axis=1)
        total = lax.dot_general(left, right, NT, preferred_element_type=jnp.float32).T
        out_ref[:, r * BLOCK : (r + 1) * BLOCK] = inv[r : r + 1] * total[:classes] + bias


def outer_aggregate(tile_col, near_tiles, stacked, arrived, degrees, bias):
    row_blocks = near_tiles.shape[0]
    peers, padded, _ = arrived.shape
    return pl.pallas_call(
        outer_kernel,
        in_specs=[pl.BlockSpec(memory_space=pltpu.SMEM)] + [whole()] * 5,
        out_specs=whole(),
        out_shape=jax.ShapeDtypeStruct((bias.shape[1], row_blocks * BLOCK), jnp.float32),
        scratch_shapes=[pltpu.VMEM((row_blocks + peers, padded, BLOCK), jnp.bfloat16)],
        compiler_params=pltpu.CompilerParams(vmem_limit_bytes=16 * MIB),
        name="outer_aggregate",
    )(tile_col, in_vmem(near_tiles), stacked, arrived, degrees, bias)


def exchange(outgoing):
    return lax.all_to_all(outgoing, ("dom", "sub"), split_axis=0, concat_axis=0, tiled=True)


def on_device(
    features, w_inner, bias_inner, w_outer, bias_outer, tiles, tile_col, degrees, send_rows
):
    lists = send_rows[0]
    classes = w_outer.shape[1]
    padded = 16 * ((classes + 15) // 16)
    width = w_inner.shape[1]
    degree_rows = degrees.reshape(-1, BLOCK)
    outgoing, own, near_tiles = front(lists, features.T, w_inner, degree_rows, tiles)
    arrived = exchange(outgoing)
    stacked, outgoing_scores = inner_aggregate(
        tile_col,
        lists,
        near_tiles,
        own.reshape(-1, BLOCK, width),
        arrived,
        degree_rows,
        bias_inner[None, :],
        w_outer.T,
        padded,
    )
    arrived_scores = exchange(outgoing_scores)
    logits_t = outer_aggregate(
        tile_col, near_tiles, stacked, arrived_scores, degree_rows, bias_outer[None, :]
    )
    return logits_t.T


def solution(mesh):
    return jax.shard_map(
        on_device,
        mesh=mesh,
        in_specs=(
            P(("dom", "sub"), None),
            P(),
            P(),
            P(),
            P(),
            P(("dom", "sub"), None, None, None),
            P(("dom", "sub"), None),
            P(("dom", "sub")),
            P(("dom", "sub"), None, None),
        ),
        out_specs=P(("dom", "sub"), None),
        check_vma=False,
    )
```

```python
import jax
import jax.numpy as jnp
from jax import lax
from jax.experimental import pallas as pl
from jax.experimental.pallas import tpu as pltpu
from jax.sharding import PartitionSpec as P

BLOCK = 128
ROW_LISTS = 32
SCORE_LISTS = 8
QUARTER = 256
SCORE_UNROLL = 4
NT = (((1,), (1,)), ((), ()))
MIB = 2**20


def whole():
    return pl.BlockSpec(memory_space=pltpu.VMEM)


def in_hbm(array):
    return pltpu.with_memory_space_constraint(array, pltpu.HBM)


def in_vmem(array):
    return pltpu.with_memory_space_constraint(array, pltpu.VMEM)


def anywhere():
    return pl.BlockSpec(memory_space=pltpu.HBM)


def front_kernel(
    lists_ref, features_ref, w_ref, degrees_ref, tiles_ref, sent_ref, own_ref, near_ref, pick_ref, tile_sem
):
    height = own_ref.shape[0]
    fetch = pltpu.make_async_copy(tiles_ref, near_ref, tile_sem.at[0])

    @pl.when(pl.program_id(0) == 0)
    def _():
        fetch.start()
        inv = lax.rsqrt(degrees_ref[...].astype(jnp.float32)).T
        for r in range(height // BLOCK):
            part = lax.dot_general(
                features_ref[:, r * BLOCK : (r + 1) * BLOCK],
                w_ref[...],
                (((0,), (0,)), ((), ())),
                preferred_element_type=jnp.float32,
            )
            own_ref[r * BLOCK : (r + 1) * BLOCK] = (part * inv[:, r : r + 1]).astype(jnp.bfloat16)

    by_slot = lists_ref[...].T
    row_of_lane = lax.broadcasted_iota(jnp.int32, (BLOCK, height), 1)
    for p in range(ROW_LISTS):
        pick_ref[p * BLOCK : (p + 1) * BLOCK] = (
            (by_slot[:, p : p + 1] == row_of_lane).astype(jnp.float32).astype(jnp.bfloat16)
        )
    rows = jnp.dot(pick_ref[...], own_ref[...], preferred_element_type=jnp.float32)
    sent_ref[...] = rows.astype(jnp.bfloat16).reshape(sent_ref.shape)

    @pl.when(pl.program_id(0) == pl.num_programs(0) - 1)
    def _():
        fetch.wait()


def front(lists, features_t, w_inner, degrees, tiles):
    peers = lists.shape[0]
    height = features_t.shape[1]
    width = w_inner.shape[1]
    return pl.pallas_call(
        front_kernel,
        grid=(peers // ROW_LISTS,),
        in_specs=[
            pl.BlockSpec((ROW_LISTS, BLOCK), lambda g: (g, 0)),
            pl.BlockSpec(features_t.shape, lambda g: (0, 0)),
            pl.BlockSpec(w_inner.shape, lambda g: (0, 0)),
            pl.BlockSpec(degrees.shape, lambda g: (0, 0)),
            pl.BlockSpec(memory_space=pl.ANY),
        ],
        out_specs=[
            pl.BlockSpec((ROW_LISTS, BLOCK, width), lambda g: (g, 0, 0)),
            pl.BlockSpec((height, width), lambda g: (0, 0)),
            pl.BlockSpec(memory_space=pl.ANY),
        ],
        out_shape=[
            pltpu.VMEM((peers, BLOCK, width), jnp.bfloat16),
            jax.ShapeDtypeStruct((height, width), jnp.bfloat16),
            pltpu.VMEM(tiles.shape, tiles.dtype),
        ],
        scratch_shapes=[
            pltpu.VMEM((ROW_LISTS * BLOCK, height), jnp.bfloat16),
            pltpu.SemaphoreType.DMA((1,)),
        ],
        compiler_params=pltpu.CompilerParams(vmem_limit_bytes=28 * MIB),
        name="front",
    )(in_hbm(lists), in_hbm(features_t), in_hbm(w_inner), in_hbm(degrees), in_hbm(tiles))


def inner_kernel(
    cols_ref,
    lists_ref,
    tiles_ref,
    own_ref,
    arrived_ref,
    degrees_ref,
    bias_ref,
    w_ref,
    stacked_ref,
    outgoing,
    hidden,
):
    row_blocks, count = tiles_ref.shape[:2]
    own_blocks, peers = own_ref.shape[0], arrived_ref.shape[0]
    padded = outgoing.shape[1]
    classes = w_ref.shape[0]
    quarters = stacked_ref.shape[0] // padded
    steps = peers // SCORE_LISTS

    def block(c):
        near = own_ref[jnp.minimum(c, own_blocks - 1)]
        far = arrived_ref[jnp.maximum(c - own_blocks, 0)]
        return jnp.where(c < own_blocks, near, far)

    def list_row(g):
        rows = lists_ref[pl.ds(pl.multiple_of(g * SCORE_LISTS, SCORE_LISTS), SCORE_LISTS)]
        return jnp.concatenate([rows[k : k + 1] for k in range(SCORE_LISTS)], axis=1)

    row_of_sublane = lax.broadcasted_iota(jnp.int16, (QUARTER, SCORE_LISTS * BLOCK), 0)
    one = jnp.ones(row_of_sublane.shape, jnp.bfloat16)
    zero = jnp.zeros(row_of_sublane.shape, jnp.bfloat16)

    inv = lax.rsqrt(degrees_ref[...].astype(jnp.float32)).T
    for r in range(row_blocks):
        left = jnp.concatenate([tiles_ref[r, t] for t in range(count)], axis=1)
        right = jnp.concatenate([block(cols_ref[r, t]) for t in range(count)], axis=0)
        total = jnp.dot(left, right, preferred_element_type=jnp.float32)
        scale = inv[:, r : r + 1]
        row = scale * jnp.maximum(scale * total + bias_ref[...], 0.0)
        hidden[r * BLOCK : (r + 1) * BLOCK] = row.astype(jnp.bfloat16)

    scores = lax.dot_general(w_ref[...], hidden[...], NT, preferred_element_type=jnp.float32)
    scores = jnp.concatenate([scores, jnp.zeros((padded - classes, scores.shape[1]), jnp.float32)], axis=0)
    scores = scores.astype(jnp.bfloat16)
    for q in range(quarters):
        stacked_ref[q * padded : (q + 1) * padded] = scores[:, q * QUARTER : (q + 1) * QUARTER]

    @pl.loop(0, steps // SCORE_UNROLL)
    def _(h):
        for u in range(SCORE_UNROLL):
            g = h * SCORE_UNROLL + u
            quarter = jnp.right_shift(list_row(g), QUARTER.bit_length() - 1)
            low = jnp.bitwise_and(list_row(g), QUARTER - 1)
            near_row = jnp.broadcast_to(low, row_of_sublane.shape).astype(jnp.int16) == row_of_sublane
            pick = jnp.where(near_row, one, zero)
            every = jnp.dot(stacked_ref[...], pick, preferred_element_type=jnp.float32)
            chosen = jnp.zeros((padded, SCORE_LISTS * BLOCK), jnp.float32)
            for q in range(quarters):
                chosen = jnp.where(quarter == q, every[q * padded : (q + 1) * padded], chosen)
            chosen = chosen.astype(jnp.bfloat16)
            for k in range(SCORE_LISTS):
                outgoing[g * SCORE_LISTS + k] = chosen[:, k * BLOCK : (k + 1) * BLOCK]


def inner_aggregate(tile_col, lists, near_tiles, own, arrived, degrees, bias, w_t, padded):
    row_blocks = near_tiles.shape[0]
    peers, _, width = arrived.shape
    height = row_blocks * BLOCK
    return pl.pallas_call(
        inner_kernel,
        in_specs=[pl.BlockSpec(memory_space=pltpu.SMEM), whole()] + [whole()] * 6,
        out_specs=[whole(), whole()],
        out_shape=[
            jax.ShapeDtypeStruct((padded * height // QUARTER, QUARTER), jnp.bfloat16),
            pltpu.VMEM((peers, padded, BLOCK), jnp.bfloat16),
        ],
        scratch_shapes=[
            pltpu.VMEM((height, width), jnp.bfloat16),
        ],
        compiler_params=pltpu.CompilerParams(vmem_limit_bytes=20 * MIB),
        name="inner_aggregate",
    )(tile_col, lists, in_vmem(near_tiles), own, in_vmem(arrived), degrees, bias, w_t)


def outer_kernel(cols_ref, tiles_ref, stacked_ref, arrived_ref, degrees_ref, bias_ref, out_ref, space):
    row_blocks, count = tiles_ref.shape[:2]
    padded = arrived_ref.shape[1]
    classes = out_ref.shape[0]
    for r in range(row_blocks):
        quarter, side = divmod(r * BLOCK, QUARTER)
        space[r] = stacked_ref[quarter * padded : (quarter + 1) * padded, side : side + BLOCK]
    space[row_blocks:] = arrived_ref[...]
    inv = lax.rsqrt(degrees_ref[...].astype(jnp.float32))
    bias = bias_ref[...].T
    for r in range(row_blocks):
        left = jnp.concatenate([tiles_ref[r, t] for t in range(count)], axis=1)
        right = jnp.concatenate([space[cols_ref[r, t]] for t in range(count)], axis=1)
        total = lax.dot_general(left, right, NT, preferred_element_type=jnp.float32).T
        out_ref[:, r * BLOCK : (r + 1) * BLOCK] = inv[r : r + 1] * total[:classes] + bias


def outer_aggregate(tile_col, near_tiles, stacked, arrived, degrees, bias):
    row_blocks = near_tiles.shape[0]
    peers, padded, _ = arrived.shape
    return pl.pallas_call(
        outer_kernel,
        in_specs=[pl.BlockSpec(memory_space=pltpu.SMEM)] + [whole()] * 5,
        out_specs=whole(),
        out_shape=jax.ShapeDtypeStruct((bias.shape[1], row_blocks * BLOCK), jnp.float32),
        scratch_shapes=[pltpu.VMEM((row_blocks + peers, padded, BLOCK), jnp.bfloat16)],
        compiler_params=pltpu.CompilerParams(vmem_limit_bytes=16 * MIB),
        name="outer_aggregate",
    )(tile_col, in_vmem(near_tiles), stacked, arrived, degrees, bias)


def exchange(outgoing):
    return lax.all_to_all(outgoing, ("dom", "sub"), split_axis=0, concat_axis=0, tiled=True)


def on_device(
    features, w_inner, bias_inner, w_outer, bias_outer, tiles, tile_col, degrees, send_rows
):
    lists = send_rows[0]
    classes = w_outer.shape[1]
    padded = 16 * ((classes + 15) // 16)
    width = w_inner.shape[1]
    degree_rows = degrees.reshape(-1, BLOCK)
    outgoing, own, near_tiles = front(lists, features.T, w_inner, degree_rows, tiles)
    arrived = exchange(outgoing)
    stacked, outgoing_scores = inner_aggregate(
        tile_col,
        lists,
        near_tiles,
        own.reshape(-1, BLOCK, width),
        arrived,
        degree_rows,
        bias_inner[None, :],
        w_outer.T,
        padded,
    )
    arrived_scores = exchange(outgoing_scores)
    logits_t = outer_aggregate(
        tile_col, near_tiles, stacked, arrived_scores, degree_rows, bias_outer[None, :]
    )
    return logits_t.T


def solution(mesh):
    return jax.shard_map(
        on_device,
        mesh=mesh,
        in_specs=(
            P(("dom", "sub"), None),
            P(),
            P(),
            P(),
            P(),
            P(("dom", "sub"), None, None, None),
            P(("dom", "sub"), None),
            P(("dom", "sub")),
            P(("dom", "sub"), None, None),
        ),
        out_specs=P(("dom", "sub"), None),
        check_vma=False,
    )
```

```python
import jax
import jax.numpy as jnp
from jax import lax
from jax.experimental import pallas as pl
from jax.experimental.pallas import tpu as pltpu
from jax.sharding import PartitionSpec as P

BLOCK = 128
ROW_LISTS = 64
SCORE_LISTS = 8
QUARTER = 256
SCORE_UNROLL = 4
NT = (((1,), (1,)), ((), ()))
MIB = 2**20


def whole():
    return pl.BlockSpec(memory_space=pltpu.VMEM)


def in_hbm(array):
    return pltpu.with_memory_space_constraint(array, pltpu.HBM)


def in_vmem(array):
    return pltpu.with_memory_space_constraint(array, pltpu.VMEM)


def anywhere():
    return pl.BlockSpec(memory_space=pltpu.HBM)


def front_kernel(
    lists_ref, features_ref, w_ref, degrees_ref, tiles_ref, sent_ref, own_ref, near_ref, pick_ref, tile_sem
):
    height = own_ref.shape[0]
    fetch = pltpu.make_async_copy(tiles_ref, near_ref, tile_sem.at[0])
    fetch.start()
    inv = lax.rsqrt(degrees_ref[...].astype(jnp.float32)).T
    for r in range(height // BLOCK):
        part = lax.dot_general(
            features_ref[:, r * BLOCK : (r + 1) * BLOCK],
            w_ref[...],
            (((0,), (0,)), ((), ())),
            preferred_element_type=jnp.float32,
        )
        own_ref[r * BLOCK : (r + 1) * BLOCK] = (part * inv[:, r : r + 1]).astype(jnp.bfloat16)

    row_of_lane = lax.broadcasted_iota(jnp.int32, (BLOCK, height), 1)

    @pl.loop(0, sent_ref.shape[0] // ROW_LISTS)
    def _(g):
        here = pl.ds(pl.multiple_of(g * ROW_LISTS, ROW_LISTS), ROW_LISTS)
        by_slot = lists_ref[here].T
        for p in range(ROW_LISTS):
            pick_ref[p * BLOCK : (p + 1) * BLOCK] = (
                (by_slot[:, p : p + 1] == row_of_lane).astype(jnp.float32).astype(jnp.bfloat16)
            )
        rows = jnp.dot(pick_ref[...], own_ref[...], preferred_element_type=jnp.float32)
        sent_ref[here] = rows.astype(jnp.bfloat16).reshape(ROW_LISTS, BLOCK, rows.shape[1])

    fetch.wait()


def front(lists, features_t, w_inner, degrees, tiles):
    peers = lists.shape[0]
    height = features_t.shape[1]
    width = w_inner.shape[1]
    return pl.pallas_call(
        front_kernel,
        in_specs=[whole()] * 4 + [anywhere()],
        out_specs=[whole(), whole(), pl.BlockSpec(memory_space=pl.ANY)],
        out_shape=[
            pltpu.VMEM((peers, BLOCK, width), jnp.bfloat16),
            jax.ShapeDtypeStruct((height, width), jnp.bfloat16),
            pltpu.VMEM(tiles.shape, tiles.dtype),
        ],
        scratch_shapes=[
            pltpu.VMEM((ROW_LISTS * BLOCK, height), jnp.bfloat16),
            pltpu.SemaphoreType.DMA((1,)),
        ],
        compiler_params=pltpu.CompilerParams(vmem_limit_bytes=36 * MIB),
        name="front",
    )(in_hbm(lists), in_hbm(features_t), in_hbm(w_inner), in_hbm(degrees), in_hbm(tiles))


def inner_kernel(
    cols_ref,
    lists_ref,
    tiles_ref,
    own_ref,
    arrived_ref,
    degrees_ref,
    bias_ref,
    w_ref,
    stacked_ref,
    outgoing,
    hidden,
):
    row_blocks, count = tiles_ref.shape[:2]
    own_blocks, peers = own_ref.shape[0], arrived_ref.shape[0]
    padded = outgoing.shape[1]
    classes = w_ref.shape[0]
    quarters = stacked_ref.shape[0] // padded
    steps = peers // SCORE_LISTS

    def block(c):
        near = own_ref[jnp.minimum(c, own_blocks - 1)]
        far = arrived_ref[jnp.maximum(c - own_blocks, 0)]
        return jnp.where(c < own_blocks, near, far)

    def list_row(g):
        rows = lists_ref[pl.ds(pl.multiple_of(g * SCORE_LISTS, SCORE_LISTS), SCORE_LISTS)]
        return jnp.concatenate([rows[k : k + 1] for k in range(SCORE_LISTS)], axis=1)

    row_of_sublane = lax.broadcasted_iota(jnp.int16, (QUARTER, SCORE_LISTS * BLOCK), 0)
    one = jnp.ones(row_of_sublane.shape, jnp.bfloat16)
    zero = jnp.zeros(row_of_sublane.shape, jnp.bfloat16)

    inv = lax.rsqrt(degrees_ref[...].astype(jnp.float32)).T
    for r in range(row_blocks):
        left = jnp.concatenate([tiles_ref[r, t] for t in range(count)], axis=1)
        right = jnp.concatenate([block(cols_ref[r, t]) for t in range(count)], axis=0)
        total = jnp.dot(left, right, preferred_element_type=jnp.float32)
        scale = inv[:, r : r + 1]
        row = scale * jnp.maximum(scale * total + bias_ref[...], 0.0)
        hidden[r * BLOCK : (r + 1) * BLOCK] = row.astype(jnp.bfloat16)

    scores = lax.dot_general(w_ref[...], hidden[...], NT, preferred_element_type=jnp.float32)
    scores = jnp.concatenate([scores, jnp.zeros((padded - classes, scores.shape[1]), jnp.float32)], axis=0)
    scores = scores.astype(jnp.bfloat16)
    for q in range(quarters):
        stacked_ref[q * padded : (q + 1) * padded] = scores[:, q * QUARTER : (q + 1) * QUARTER]

    @pl.loop(0, steps // SCORE_UNROLL)
    def _(h):
        for u in range(SCORE_UNROLL):
            g = h * SCORE_UNROLL + u
            quarter = jnp.right_shift(list_row(g), QUARTER.bit_length() - 1)
            low = jnp.bitwise_and(list_row(g), QUARTER - 1)
            near_row = jnp.broadcast_to(low, row_of_sublane.shape).astype(jnp.int16) == row_of_sublane
            pick = jnp.where(near_row, one, zero)
            every = jnp.dot(stacked_ref[...], pick, preferred_element_type=jnp.float32)
            chosen = jnp.zeros((padded, SCORE_LISTS * BLOCK), jnp.float32)
            for q in range(quarters):
                chosen = jnp.where(quarter == q, every[q * padded : (q + 1) * padded], chosen)
            chosen = chosen.astype(jnp.bfloat16)
            for k in range(SCORE_LISTS):
                outgoing[g * SCORE_LISTS + k] = chosen[:, k * BLOCK : (k + 1) * BLOCK]


def inner_aggregate(tile_col, lists, near_tiles, own, arrived, degrees, bias, w_t, padded):
    row_blocks = near_tiles.shape[0]
    peers, _, width = arrived.shape
    height = row_blocks * BLOCK
    return pl.pallas_call(
        inner_kernel,
        in_specs=[pl.BlockSpec(memory_space=pltpu.SMEM), whole()] + [whole()] * 6,
        out_specs=[whole(), whole()],
        out_shape=[
            jax.ShapeDtypeStruct((padded * height // QUARTER, QUARTER), jnp.bfloat16),
            pltpu.VMEM((peers, padded, BLOCK), jnp.bfloat16),
        ],
        scratch_shapes=[
            pltpu.VMEM((height, width), jnp.bfloat16),
        ],
        compiler_params=pltpu.CompilerParams(vmem_limit_bytes=20 * MIB),
        name="inner_aggregate",
    )(tile_col, lists, in_vmem(near_tiles), own, in_vmem(arrived), degrees, bias, w_t)


def outer_kernel(cols_ref, tiles_ref, stacked_ref, arrived_ref, degrees_ref, bias_ref, out_ref, space):
    row_blocks, count = tiles_ref.shape[:2]
    padded = arrived_ref.shape[1]
    classes = out_ref.shape[0]
    for r in range(row_blocks):
        quarter, side = divmod(r * BLOCK, QUARTER)
        space[r] = stacked_ref[quarter * padded : (quarter + 1) * padded, side : side + BLOCK]
    space[row_blocks:] = arrived_ref[...]
    inv = lax.rsqrt(degrees_ref[...].astype(jnp.float32))
    bias = bias_ref[...].T
    for r in range(row_blocks):
        left = jnp.concatenate([tiles_ref[r, t] for t in range(count)], axis=1)
        right = jnp.concatenate([space[cols_ref[r, t]] for t in range(count)], axis=1)
        total = lax.dot_general(left, right, NT, preferred_element_type=jnp.float32).T
        out_ref[:, r * BLOCK : (r + 1) * BLOCK] = inv[r : r + 1] * total[:classes] + bias


def outer_aggregate(tile_col, near_tiles, stacked, arrived, degrees, bias):
    row_blocks = near_tiles.shape[0]
    peers, padded, _ = arrived.shape
    return pl.pallas_call(
        outer_kernel,
        in_specs=[pl.BlockSpec(memory_space=pltpu.SMEM)] + [whole()] * 5,
        out_specs=whole(),
        out_shape=jax.ShapeDtypeStruct((bias.shape[1], row_blocks * BLOCK), jnp.float32),
        scratch_shapes=[pltpu.VMEM((row_blocks + peers, padded, BLOCK), jnp.bfloat16)],
        compiler_params=pltpu.CompilerParams(vmem_limit_bytes=16 * MIB),
        name="outer_aggregate",
    )(tile_col, in_vmem(near_tiles), stacked, arrived, degrees, bias)


def exchange(outgoing):
    return lax.all_to_all(outgoing, ("dom", "sub"), split_axis=0, concat_axis=0, tiled=True)


def on_device(
    features, w_inner, bias_inner, w_outer, bias_outer, tiles, tile_col, degrees, send_rows
):
    lists = send_rows[0]
    classes = w_outer.shape[1]
    padded = 16 * ((classes + 15) // 16)
    width = w_inner.shape[1]
    degree_rows = degrees.reshape(-1, BLOCK)
    outgoing, own, near_tiles = front(lists, features.T, w_inner, degree_rows, tiles)
    arrived = exchange(outgoing)
    stacked, outgoing_scores = inner_aggregate(
        tile_col,
        lists,
        near_tiles,
        own.reshape(-1, BLOCK, width),
        arrived,
        degree_rows,
        bias_inner[None, :],
        w_outer.T,
        padded,
    )
    arrived_scores = exchange(outgoing_scores)
    logits_t = outer_aggregate(
        tile_col, near_tiles, stacked, arrived_scores, degree_rows, bias_outer[None, :]
    )
    return logits_t.T


def solution(mesh):
    return jax.shard_map(
        on_device,
        mesh=mesh,
        in_specs=(
            P(("dom", "sub"), None),
            P(),
            P(),
            P(),
            P(),
            P(("dom", "sub"), None, None, None),
            P(("dom", "sub"), None),
            P(("dom", "sub")),
            P(("dom", "sub"), None, None),
        ),
        out_specs=P(("dom", "sub"), None),
        check_vma=False,
    )
```
